32 devices in a mesh: blk: 4 (over x, core), uly: 8 (over z, y).
Axes of the slice: x: 2, y: 2, z: 4, core: 2. Of those that a mesh axis runs over, the one named last changes fastest.
Arguments:
- query: bfloat16 [4096, 4096], P(('blk', 'uly')), may hold values from -5 to 5
- key_input: bfloat16 [4096, 512], P(('blk', 'uly')), may hold values from -5 to 5
- value_input: bfloat16 [4096, 512], P(('blk', 'uly')), may hold values from -6 to 6
- output: bfloat16 [4096, 4096], P(('blk', 'uly')), may hold values from -6 to 6
- out_grad: bfloat16 [4096, 4096], P(('blk', 'uly')), may hold values from -6 to 6
Outputs:
- query_grad: bfloat16 [4096, 4096], P(('blk', 'uly'))
- key_gradient: bfloat16 [4096, 512], P(('blk', 'uly'))
- value_gradient: bfloat16 [4096, 512], P(('blk', 'uly'))
The draws below stay inside these ranges and needn't reach their ends.
All inputs are finite; a program needn't handle non-finite values.
Results may differ from the reference program's by a relative error of at most 0.009.
Values may be sent and summed in bfloat16 or wider, within the bound.
No kernel may reach another device: no remote copies, remote signals or barrier semaphores. Data moves between devices by JAX's collectives and lax.ppermute only.
A program may use at most 64 MiB of HBM per device.

```python
import jax
import jax.numpy as jnp
from jax import lax

QUERY_HEADS = 32
KEY_VALUE_HEADS = 4
HEAD_SIZE = 128
WINDOW_KEYS = 1024
SEQUENCE_TOKENS = 4096


def draw_query(key, part):
    start_offset = jnp.clip(jax.random.normal(jax.random.fold_in(key, 1), (SEQUENCE_TOKENS, QUERY_HEADS * HEAD_SIZE), jnp.float32), -5.0, 5.0)
    return start_offset.astype(jnp.bfloat16)


def draw_key_input(key, part):
    start_offset = jnp.clip(jax.random.normal(jax.random.fold_in(key, 5), (SEQUENCE_TOKENS, KEY_VALUE_HEADS * HEAD_SIZE), jnp.float32), -5.0, 5.0)
    return start_offset.astype(jnp.bfloat16)


def block_scale(key, extent, pieces, least, top_value):
    loudness, own = 1.0, jax.random.fold_in(key, 6)
    for position, parts in pieces:
        heights = jnp.exp(jax.random.uniform(jax.random.fold_in(own, position), (parts,), jnp.float32, least / len(pieces), top_value / len(pieces)))
        loudness = loudness * jnp.repeat(heights, extent[position] // parts).reshape([-1 if axis == position else 1 for axis in range(len(extent))])
    return loudness


def gaussian(key, shape, scale, limit, cuts=(), kind=jnp.bfloat16):
    drawn = jax.random.normal(key, shape, jnp.float32) * scale
    if len(cuts) > 0:
        drawn = block_scale(key, shape, cuts, -0.22, 0.18) * drawn
    return jnp.clip(drawn, min=-limit, max=limit).astype(kind)


def setup_inputs(seed: int = 0) -> dict:
    streams_of = jax.random.split(jax.random.key(seed), 6)
    query = draw_query(jax.random.fold_in(streams_of[5], 71), 0)
    key_input = draw_key_input(jax.random.fold_in(streams_of[5], 71), 0)
    value_input = gaussian(streams_of[2], (SEQUENCE_TOKENS, KEY_VALUE_HEADS * HEAD_SIZE), 1.0, 6.0, ((0, 32),))
    output = gaussian(streams_of[3], (SEQUENCE_TOKENS, QUERY_HEADS * HEAD_SIZE), 1.0, 6.0, ((0, 32),))
    out_grad = gaussian(streams_of[4], (SEQUENCE_TOKENS, QUERY_HEADS * HEAD_SIZE), 1.0, 6.0, ((0, 32),))
    return dict(query=query, key_input=key_input, value_input=value_input, output=output, out_grad=out_grad)


def reference(query, key_input, value_input, output, out_grad):
    scaling = HEAD_SIZE ** -0.5
    group_width = QUERY_HEADS // KEY_VALUE_HEADS
    block = min(512, SEQUENCE_TOKENS)
    block_count = SEQUENCE_TOKENS // block
    span = WINDOW_KEYS + block
    highest = lax.Precision.HIGHEST
    query_heads = query.reshape(SEQUENCE_TOKENS, QUERY_HEADS, HEAD_SIZE).transpose(1, 0, 2)
    output_heads = output.reshape(SEQUENCE_TOKENS, QUERY_HEADS, HEAD_SIZE).transpose(1, 0, 2)
    grad_heads = out_grad.reshape(SEQUENCE_TOKENS, QUERY_HEADS, HEAD_SIZE).transpose(1, 0, 2)
    key_head_rows = jnp.pad(key_input.reshape(SEQUENCE_TOKENS, KEY_VALUE_HEADS, HEAD_SIZE).transpose(1, 0, 2), ((0, 0), (WINDOW_KEYS, 0), (0, 0)))
    value_head_rows = jnp.pad(value_input.reshape(SEQUENCE_TOKENS, KEY_VALUE_HEADS, HEAD_SIZE).transpose(1, 0, 2), ((0, 0), (WINDOW_KEYS, 0), (0, 0)))
    offsets = jnp.arange(block, dtype=jnp.int32)[:, None]
    columns = jnp.arange(span, dtype=jnp.int32)[None, :]
    relative = columns - offsets
    inside = (relative >= 1) & (relative <= WINDOW_KEYS)

    def group_member_count(group):
        key_pad = key_head_rows[group].astype(jnp.float32)
        value_pad = value_head_rows[group].astype(jnp.float32)

        def per_head(carry, member):
            key_acc, value_acc = carry
            head = group * group_width + member
            query_wide = query_heads[head].astype(jnp.float32)
            grad_wide = grad_heads[head].astype(jnp.float32)
            row_dot = jnp.sum(output_heads[head].astype(jnp.float32) * grad_wide, axis=1)

            def per_block(inner, index):
                key_acc, value_acc = inner
                start = (index * block).astype(jnp.int32)
                query_block = lax.dynamic_slice_in_dim(query_wide, start, block, 0)
                grad_block = lax.dynamic_slice_in_dim(grad_wide, start, block, 0)
                dot_block = lax.dynamic_slice_in_dim(row_dot, start, block, 0)
                key_block = lax.dynamic_slice_in_dim(key_pad, start, span, 0)
                value_block = lax.dynamic_slice_in_dim(value_pad, start, span, 0)
                visible = inside & (start - WINDOW_KEYS + columns >= 0)
                scores = jnp.dot(query_block, key_block.T, precision=highest) * scaling
                masked = jnp.where(visible, scores, -1e30)
                row_max = jnp.max(masked, axis=1)
                row_sum = jnp.sum(jnp.where(visible, jnp.exp(masked - row_max[:, None]), 0.0), axis=1)
                log_total = row_max + jnp.log(row_sum)
                weights = jnp.where(visible, jnp.exp(masked - log_total[:, None]), 0.0)
                weights_low = weights.astype(jnp.bfloat16).astype(jnp.float32)
                weight_grad = jnp.dot(grad_block, value_block.T, precision=highest)
                score_grad = (weights * (weight_grad - dot_block[:, None]) * scaling).astype(jnp.bfloat16)
                score_wide = score_grad.astype(jnp.float32)
                query_portion = jnp.dot(score_wide, key_block, precision=highest)
                key_portion = jnp.dot(score_wide.T, query_block, precision=highest)
                value_portion = jnp.dot(weights_low.T, grad_block, precision=highest)
                key_acc = lax.dynamic_update_slice_in_dim(
                    key_acc, lax.dynamic_slice_in_dim(key_acc, start, span, 0) + key_portion, start, 0)
                value_acc = lax.dynamic_update_slice_in_dim(
                    value_acc, lax.dynamic_slice_in_dim(value_acc, start, span, 0) + value_portion, start, 0)
                return (key_acc, value_acc), query_portion

            (key_acc, value_acc), query_parts = lax.scan(
                per_block, (key_acc, value_acc), jnp.arange(block_count, dtype=jnp.int32))
            return (key_acc, value_acc), query_parts.reshape(SEQUENCE_TOKENS, HEAD_SIZE).astype(jnp.bfloat16)

        zeros = jnp.zeros((SEQUENCE_TOKENS + WINDOW_KEYS, HEAD_SIZE), jnp.float32)
        (key_acc, value_acc), query_portion = lax.scan(
            per_head, (zeros, zeros), jnp.arange(group_width, dtype=jnp.int32))
        return query_portion, key_acc[WINDOW_KEYS:], value_acc[WINDOW_KEYS:]

    query_portion, key_portion, value_portion = lax.map(group_member_count, jnp.arange(KEY_VALUE_HEADS, dtype=jnp.int32))
    query_grad = query_portion.reshape(QUERY_HEADS, SEQUENCE_TOKENS, HEAD_SIZE).transpose(1, 0, 2).reshape(SEQUENCE_TOKENS, QUERY_HEADS * HEAD_SIZE)
    key_gradient = key_portion.transpose(1, 0, 2).reshape(SEQUENCE_TOKENS, KEY_VALUE_HEADS * HEAD_SIZE).astype(jnp.bfloat16)
    value_gradient = value_portion.transpose(1, 0, 2).reshape(SEQUENCE_TOKENS, KEY_VALUE_HEADS * HEAD_SIZE).astype(jnp.bfloat16)
    return (query_grad, key_gradient, value_gradient)
```

```python
import functools
import math

import jax
import jax.numpy as jnp
from jax import lax
from jax.experimental import pallas as pl
from jax.experimental.pallas import tpu as pltpu
from jax.sharding import PartitionSpec as P

KV_HEADS = 4
WINDOW = 1024
AXES = ("blk", "uly")
F32, BF16 = jnp.float32, jnp.bfloat16
VMEM = pl.BlockSpec(memory_space=pltpu.VMEM)
SMEM = pl.BlockSpec(memory_space=pltpu.SMEM)
NEG = -1e30


def call(body, args, outs, scratch=(), flops=0, name=None):
    size = sum(math.prod(a.shape) * a.dtype.itemsize for a in args)
    size += sum(math.prod(o.shape) * o.dtype.itemsize for o in outs)
    return pl.pallas_call(
        body,
        out_shape=tuple(outs),
        in_specs=[SMEM] + [VMEM] * (len(args) - 1),
        out_specs=tuple(VMEM for _ in outs),
        scratch_shapes=list(scratch),
        compiler_params=pltpu.CompilerParams(vmem_limit_bytes=56 * 2**20),
        cost_estimate=pl.CostEstimate(flops=flops, bytes_accessed=size, transcendentals=0),
        name=name,
    )(*args)


def shape(dims, dtype=BF16):
    return jax.ShapeDtypeStruct(dims, dtype)


def lanes(index, size):
    return pl.ds(pl.multiple_of(index * size, size), size)


def kv_prep(meta, key, value, *outs):
    d = key.shape[1] // KV_HEADS
    for k, out in enumerate(outs):
        h = meta[0] ^ k
        out[:, :d] = key[:, lanes(h, d)]
        out[:, d:] = value[:, lanes(h, d)]


def kv_collect(meta, *refs):
    parts, (kp, vp) = refs[:KV_HEADS], refs[KV_HEADS:]
    t, d = parts[0].shape[0], parts[0].shape[1] // 2
    for k, part in enumerate(parts):
        s = meta[0] ^ k
        kp[lanes(s, t), :] = part[:, :d]
        vp[lanes(s, t), :] = part[:, d:]


def q_prep(meta, query, *outs):
    w = query.shape[1] // KV_HEADS
    for k, out in enumerate(outs):
        out[...] = query[:, lanes(meta[0] ^ k, w)]


def o_prep(meta, output, grad, *refs):
    g_out, d_out, dots = refs[:KV_HEADS], refs[KV_HEADS:-1], refs[-1]
    w = grad.shape[1] // KV_HEADS
    t, d = dots.shape
    heads = grad.shape[1] // d
    column = lax.broadcasted_iota(jnp.int32, (t, d), 1)
    acc = jnp.zeros((t, d), F32)
    for h in range(heads):
        cut = slice(h * d, (h + 1) * d)
        product = output[:, cut].astype(F32) * grad[:, cut].astype(F32)
        acc = jnp.where(column == h, jnp.sum(product, axis=1, keepdims=True), acc)
    dots[...] = acc.T
    for k in range(KV_HEADS):
        h = meta[0] ^ k
        g_out[k][...] = grad[:, lanes(h, w)]
        d_out[k][...] = dots[lanes(h, heads // KV_HEADS), :]


def gather_rows(meta, parts, dest):
    t, d = dest.shape[1] // (parts[0].shape[1] // dest.shape[2]), dest.shape[2]
    for k, part in enumerate(parts):
        s = meta[0] ^ k
        for h in range(part.shape[1] // d):
            dest[s, h * t : (h + 1) * t, :] = part[:, h * d : (h + 1) * d]


def window_rows(meta, pieces, prev, ext):
    z, n, half = meta[1], len(pieces), pieces[0].shape[0] // 2
    steps = ext.shape[1] // half
    for j in range(steps):
        own, m = z >= j, j % n
        at = slice((steps - 1 - j) * half, (steps - j) * half)
        first, second = pieces[m][:half, :], pieces[m][half:, :]
        ext[0, at, :] = jnp.where(own, first, prev[m * half : (m + 1) * half, :])
        ext[1, at, :] = jnp.where(own, second, first)


def unwindow_rows(meta, acc, scale, pieces, prev):
    z, n, half = meta[1], len(pieces), pieces[0].shape[0] // 2
    steps = acc.shape[1] // half
    for m in range(n):
        zero = jnp.zeros((half, acc.shape[2]), F32)
        first = second = back = zero
        for j in range(m, steps, n):
            own = z >= j
            at = slice((steps - 1 - j) * half, (steps - j) * half)
            a, b = acc[0, at, :], acc[1, at, :]
            first = first + jnp.where(own, a, b)
            second = second + jnp.where(own, b, zero)
            back = back + jnp.where(own, zero, a)
        pieces[m][:half, :] = first * scale
        pieces[m][half:, :] = second * scale
        prev[m * half : (m + 1) * half, :] = (back * scale).astype(prev.dtype)


NT = (((1,), (1,)), ((), ()))
NN = (((1,), (0,)), ((), ()))


def dot(a, b, dims):
    return lax.dot_general(a, b, dims, preferred_element_type=F32)


def scores_of(meta, s, keys, queries, t):
    raw = dot(keys, queries, NT)
    row = lax.broadcasted_iota(jnp.int32, (t, queries.shape[0]), 0)
    col = lax.broadcasted_iota(jnp.int32, (t, queries.shape[0]), 1) % t
    count = keys.shape[0] // t
    out = []
    for c in range(count):
        part = raw[c * t : (c + 1) * t]
        if c == 0:
            part = jnp.where(row > col, part, NEG)
        if c == count - 1:
            part = jnp.where(row <= col, part, NEG)
        else:
            part = part + jnp.where(meta[2 + s] + c >= 0, 0.0, NEG)
        out.append(part)
    return out


def first_pass(n, factor, meta, *refs):
    q_in, g_in, refs = refs[:4], refs[4:8], refs[8:]
    pieces, prev, refs = refs[:n], refs[n], refs[n + 1 :]
    dv, dv_prev, lse = refs[:n], refs[n], refs[n + 1]
    qs, gs, ext, acc = refs[n + 2 :]
    gather_rows(meta, q_in, qs)
    gather_rows(meta, g_in, gs)
    window_rows(meta, pieces, prev, ext)
    acc[...] = jnp.zeros_like(acc)
    t, d = ext.shape[2], ext.shape[2]
    t = q_in[0].shape[0]
    span = WINDOW + t
    two = 2 * t
    pairs = qs.shape[1] // two

    def step(i, _):
        s, hp = i // pairs, i % pairs
        run, at = s // 2, pl.ds(pl.multiple_of((s % 2) * t, t), span)
        rows = lanes(hp, two)
        sc = scores_of(meta, s, ext[run, at, :], qs[s, rows, :], t)
        top = functools.reduce(jnp.maximum, [jnp.max(x, axis=0, keepdims=True) for x in sc])
        ex = [jnp.exp2((x - top) * factor) for x in sc]
        total = functools.reduce(jnp.add, [jnp.sum(x, axis=0, keepdims=True) for x in ex])
        inv = 1.0 / total
        weights = jnp.concatenate([(x * inv).astype(BF16) for x in ex], axis=0)
        acc[run, at, :] += dot(weights, gs[s, rows, :], NN)
        lse[pl.ds(i, 1), :] = top * factor + jnp.log2(total)
        return 0

    lax.fori_loop(0, 4 * pairs, step, 0)
    unwindow_rows(meta, acc, 1.0, dv, dv_prev)


def second_pass(n, factor, scaling, meta, *refs):
    q_in, g_in, d_in, refs = refs[:4], refs[4:8], refs[8:12], refs[12:]
    lse, refs = refs[0], refs[1:]
    k_pieces, k_prev, refs = refs[:n], refs[n], refs[n + 1 :]
    v_pieces, v_prev, refs = refs[:n], refs[n], refs[n + 1 :]
    dk, dk_prev, dq_out, refs = refs[:n], refs[n], refs[n + 1 : n + 5], refs[n + 5 :]
    qs, gs, kext, vext, kt, acc, dots, dq = refs
    gather_rows(meta, q_in, qs)
    gather_rows(meta, g_in, gs)
    window_rows(meta, k_pieces, k_prev, kext)
    window_rows(meta, v_pieces, v_prev, vext)
    t = q_in[0].shape[0]
    span = WINDOW + t
    two = 2 * t
    pairs = qs.shape[1] // two
    for run in range(2):
        for b in range(kext.shape[1] // t):
            cut = slice(b * t, (b + 1) * t)
            kt[run, :, cut] = kext[run, cut, :].astype(F32).T.astype(BF16)
    for k in range(4):
        for h in range(2 * pairs):
            dots[(meta[0] ^ k) * pairs + h // 2, :, (h % 2) * t : (h % 2 + 1) * t] = d_in[k][h : h + 1, :]
    acc[...] = jnp.zeros_like(acc)

    def step(i, _):
        s, hp = i // pairs, i % pairs
        run, at = s // 2, pl.ds(pl.multiple_of((s % 2) * t, t), span)
        rows = lanes(hp, two)
        queries, grads = qs[s, rows, :], gs[s, rows, :]
        sc = scores_of(meta, s, kext[run, at, :], queries, t)
        norm = lse[pl.ds(i, 1), :]
        wg = dot(vext[run, at, :], grads, NT)
        dd = dots[i]
        ds = [
            (jnp.exp2(x * factor - norm) * (wg[c * t : (c + 1) * t] - dd)).astype(BF16)
            for c, x in enumerate(sc)
        ]
        ds = jnp.concatenate(ds, axis=0)
        acc[run, at, :] += dot(ds, queries, NN)
        dqt = dot(kt[run, :, at], ds, NN) * scaling
        for h in range(2):
            dq[s, hp, :, h * t : (h + 1) * t] = dqt[:, h * t : (h + 1) * t].T.astype(BF16)
        return 0

    lax.fori_loop(0, 4 * pairs, step, 0)
    unwindow_rows(meta, acc, scaling, dk, dk_prev)
    for k, out in enumerate(dq_out):
        for hp in range(pairs):
            out[:, hp * two : (hp + 1) * two] = dq[meta[0] ^ k, hp]


def reduce_parts(n, meta, *refs):
    k_parts, v_parts, outs = refs[:n], refs[n : 2 * n], refs[2 * n :]
    t = outs[0].shape[0]
    d = k_parts[0].shape[1]
    for k, out in enumerate(outs):
        at = lanes(meta[0] ^ k, t)
        out[:, :d] = sum(p[at, :].astype(F32) for p in k_parts).astype(BF16)
        out[:, d:] = sum(p[at, :].astype(F32) for p in v_parts).astype(BF16)


def finish(meta, *refs):
    q_parts, kv_parts, (dq, dk, dv) = refs[:4], refs[4:8], refs[8:]
    w, d = q_parts[0].shape[1], kv_parts[0].shape[1] // 2
    for k in range(4):
        h = meta[0] ^ k
        dq[:, lanes(h, w)] = q_parts[k][...]
        dk[:, lanes(h, d)] = kv_parts[k][:, :d]
        dv[:, lanes(h, d)] = kv_parts[k][:, d:]


def local(query, key_input, value_input, output, out_grad):
    blocks, count = lax.axis_size("blk"), lax.axis_size("uly")
    t, width = query.shape
    kv = key_input.shape[1]
    d = kv // KV_HEADS
    group = width // kv
    zs = count // 2
    reach = WINDOW // (2 * t)
    n = min(zs, reach + 1)
    pairs = group // 2
    wide = group * d
    scaling = d**-0.5
    factor = scaling * math.log2(math.e)
    b, u = lax.axis_index("blk"), lax.axis_index("uly")
    cid = (b % 2) * 2 + u % 2
    z = u // 2
    first = [((b // 2) * 2 + s // 2) * count + 2 * z + s % 2 - WINDOW // t for s in range(4)]
    meta = jnp.stack([cid, z, *first]).astype(jnp.int32)

    def device(bb, uu):
        return bb * count + uu

    def permute(value, move):
        pairs_ = []
        for bb in range(blocks):
            for uu in range(count):
                to = move(bb, uu)
                if 0 <= to[0] < blocks:
                    pairs_.append((device(bb, uu), device(*to)))
        return lax.ppermute(value, AXES, pairs_)

    def swap(parts):
        return [parts[0]] + [
            permute(parts[k], lambda bb, uu, k=k: (bb ^ (k >> 1), uu ^ (k & 1))) for k in range(1, 4)
        ]

    def along_z(piece, m):
        return permute(piece, lambda bb, uu: (bb, (uu + 2 * m) % count))

    def forward(value, step):
        return permute(value, lambda bb, uu: (bb + 2 * step, uu))

    kv_send = call(kv_prep, (meta, key_input, value_input), [shape((t, 2 * d))] * 4, name="kv_prep")
    q_send = call(q_prep, (meta, query), [shape((t, wide))] * 4, name="q_prep")
    o_send = call(
        o_prep,
        (meta, output, out_grad),
        [shape((t, wide))] * 4 + [shape((group, t), F32)] * 4,
        [pltpu.VMEM((t, d), F32)],
        name="o_prep",
    )
    kv_parts = swap(kv_send)
    k_own, v_own = call(kv_collect, (meta, *kv_parts), [shape((4 * t, d))] * 2, name="kv_collect")
    q_parts = swap(q_send)
    k_pieces = [k_own] + [along_z(k_own, m) for m in range(1, n)]
    g_parts = swap(o_send[:4])
    v_pieces = [v_own] + [along_z(v_own, m) for m in range(1, n)]
    k_prev = forward(jnp.concatenate([p[2 * t :] for p in k_pieces], axis=0), 1)
    d_parts = swap(o_send[4:])
    v_prev = forward(jnp.concatenate([p[2 * t :] for p in v_pieces], axis=0), 1)

    ext = (2, WINDOW + 2 * t, d)
    stack = pltpu.VMEM((4, group * t, d), BF16)
    work = 4 * group * t * (WINDOW + t) * d * 2
    part_shapes = [shape((4 * t, d), F32)] * n + [shape((n * 2 * t, d))]
    res = call(
        functools.partial(first_pass, n, factor),
        (meta, *q_parts, *g_parts, *k_pieces, k_prev),
        part_shapes + [shape((4 * pairs, 2 * t), F32)],
        [stack, stack, pltpu.VMEM(ext, BF16), pltpu.VMEM(ext, F32)],
        flops=2 * work,
        name="first_pass",
    )
    dv_own, dv_prev, lse = res[:n], res[n], res[n + 1]
    res = call(
        functools.partial(second_pass, n, factor, scaling),
        (meta, *q_parts, *g_parts, *d_parts, lse, *k_pieces, k_prev, *v_pieces, v_prev),
        part_shapes + [shape((t, wide))] * 4,
        [
            stack,
            stack,
            pltpu.VMEM(ext, BF16),
            pltpu.VMEM(ext, BF16),
            pltpu.VMEM((2, d, ext[1]), BF16),
            pltpu.VMEM(ext, F32),
            pltpu.VMEM((4 * pairs, 1, 2 * t), F32),
            pltpu.VMEM((4, pairs, t, 2 * t), BF16),
        ],
        flops=4 * work,
        name="second_pass",
    )
    dk_own, dk_prev, dq_send = res[:n], res[n], res[n + 1 :]

    def collect(own, prev):
        back = forward(prev, -1).reshape(n, 2 * t, d)
        sums = [
            jnp.concatenate([own[m][: 2 * t], own[m][2 * t :] + back[m].astype(F32)], axis=0)
            for m in range(n)
        ]
        return [sums[0].astype(BF16)] + [
            along_z(sums[m].astype(BF16), -m) for m in range(1, n)
        ]

    dv_parts = collect(dv_own, dv_prev)
    dk_parts = collect(dk_own, dk_prev)
    dq_parts = swap(dq_send)
    kv_back = call(
        functools.partial(reduce_parts, n),
        (meta, *dk_parts, *dv_parts),
        [shape((t, 2 * d))] * 4,
        name="reduce_parts",
    )
    kv_back = swap(kv_back)
    return call(
        finish,
        (meta, *dq_parts, *kv_back),
        [shape((t, width)), shape((t, kv)), shape((t, kv))],
        name="finish",
    )


def solution(mesh):
    spec = P(AXES, None)
    return jax.shard_map(
        local, mesh=mesh, in_specs=(spec,) * 5, out_specs=(spec,) * 3, check_vma=False
    )
```
